32 devices in a mesh: row: 2 (over x), col: 16 (over z, y, core).
Axes of the slice: x: 2, y: 2, z: 4, core: 2. Of those that a mesh axis runs over, the one named last changes fastest.
Arguments:
- eigvecs: float32 [16384, 4096], P('row', 'col'), may hold values from -6 to 6
- v_panels: float32 [8, 16384, 256], P(None, 'row', 'col'), as said below
- t_panels: float32 [8, 256, 256], P(None, None, 'col'), as said below
Outputs:
- rotated: float32 [16384, 4096], P('row', 'col')
The draws below stay inside these ranges and needn't reach their ends.
Inputs may be any that keep to these rules, and one draw needn't show every extreme that they name: `v_panels`: in panel k, vector j is zero in rows above k * 256 + j + 1, equals 1 in that row and is dense below it. t_panels[k] is upper triangular and V_k t_panels[k] V_k^T = I minus the product of the panel's 256 Householder reflections, each I - 2 v v^T / (v^T v), taken in the order of j; its diagonal lies in (0, 2].
All inputs are finite; a program needn't handle non-finite values.
Results may differ from the reference program's by a relative error of at most 0.00015.
Values sent between devices are 32-bit elements; how exact they have to be, the bound alone decides.
No kernel may reach another device: no remote copies, remote signals or barrier semaphores. Data moves between devices by JAX's collectives and lax.ppermute only.
A program may use at most 192 MiB of HBM per device.

```python
import math
import jax
import jax.numpy as jnp
from jax import lax

ORDER = 16384
PANEL_W = 256
PANELS = 8
COLS = 4096


def householder_panels(key):
    noise = jax.random.normal(jax.random.fold_in(key, 7), (PANELS, ORDER, PANEL_W), jnp.float32) / math.sqrt(ORDER)
    rows_at = lax.broadcasted_iota(jnp.int32, (PANELS, ORDER, PANEL_W), 1)
    column_at = lax.broadcasted_iota(jnp.int32, (PANELS, ORDER, PANEL_W), 2)
    panel_at = lax.broadcasted_iota(jnp.int32, (PANELS, ORDER, PANEL_W), 0)
    unit_row = panel_at * PANEL_W + column_at + 1
    return jnp.where(rows_at > unit_row, noise, jnp.where(rows_at == unit_row, 1.0, 0.0)).astype(jnp.float32)


def draw_v_panels(key, part):
    return householder_panels(key)


def draw_t_panels(key, part):
    vectors = householder_panels(key)
    gram = jnp.einsum('knb,knc->kbc', vectors, vectors, precision=lax.Precision.HIGHEST)
    identity = jnp.eye(PANEL_W, dtype=jnp.float32)
    inverse_factor = jnp.triu(gram, 1) + 0.5 * gram * identity
    eye_stack = jnp.broadcast_to(identity, (PANELS, PANEL_W, PANEL_W))
    factor = lax.linalg.triangular_solve(inverse_factor, eye_stack, left_side=True, lower=False)
    return jnp.triu(factor).astype(jnp.float32)


def block_scale(own_key, shape, split, least, largest):
    level = 1.0
    for position, shards_of in split:
        draws = jax.random.uniform(jax.random.fold_in(jax.random.fold_in(own_key, 6), position), (shards_of,), jnp.float32, least / len(split), largest / len(split))
        level = level * jnp.repeat(jnp.exp(draws), shape[position] // shards_of).reshape((-1,) + (1,) * (len(shape) - 1 - position))
    return level


def scatter_about(rng, shape, deviation, most, pieces=(), held_as=jnp.bfloat16):
    loudness = block_scale(rng, shape, pieces, -0.22, 0.18) if pieces else 1.0
    drawn = jax.random.normal(rng, shape, jnp.float32) * deviation * loudness
    return jnp.minimum(jnp.maximum(drawn, -most), most).astype(held_as)


def setup_inputs(seed: int = 0) -> dict:
    keys = jax.random.split(jax.random.key(seed), 4)
    return {
        "eigvecs": scatter_about(keys[0], (ORDER, COLS), 1.0, 6.0, ((0, 2), (1, 16)), jnp.float32),
        "v_panels": draw_v_panels(jax.random.fold_in(keys[3], 71), 0),
        "t_panels": draw_t_panels(jax.random.fold_in(keys[3], 71), 0),
    }


def reference(eigvecs, v_panels, t_panels):
    current = eigvecs
    for panel_index in reversed(range(PANELS)):
        vectors = v_panels[panel_index]
        projected = jnp.dot(vectors.T.astype(jnp.float32), current.astype(jnp.float32), preferred_element_type=jnp.float32, precision=lax.Precision.HIGHEST)
        scaled = jnp.dot(t_panels[panel_index].astype(jnp.float32), projected.astype(jnp.float32), preferred_element_type=jnp.float32, precision=lax.Precision.HIGHEST)
        current = current - jnp.dot(vectors.astype(jnp.float32), scaled.astype(jnp.float32), preferred_element_type=jnp.float32, precision=lax.Precision.HIGHEST)
    return current
```

```python
import jax
import jax.numpy as jnp
from jax import lax
from jax.sharding import PartitionSpec as P

three_pass = lax.Precision.HIGH
GROUPS = (2, 2, 2, 1, 1)


def dot(left, right, contract):
    return lax.dot_general(
        left, right, (contract, ((), ())), precision=three_pass, preferred_element_type=jnp.float32
    )


def row_sum(partial, rows):
    if rows == 2:
        return partial + lax.ppermute(partial, "row", [(0, 1), (1, 0)])
    return lax.psum(partial, "row")


def group_sizes(panels_total):
    sizes = []
    left = panels_total
    for size in GROUPS:
        size = min(size, left)
        if size:
            sizes.append(size)
        left -= size
    while left:
        sizes.append(1)
        left -= 1
    return sizes


def solution(mesh):
    rows = mesh.shape["row"]

    def local(eigvecs, v_panels, t_panels):
        panels_total, height, _ = v_panels.shape
        groups = []
        high = panels_total
        for size in group_sizes(panels_total):
            low = high - size
            packed = jnp.concatenate([v_panels[low:high], t_panels[low:high]], axis=1)
            groups.append((low, high, lax.all_gather(packed, "col", axis=2, tiled=True)))
            high = low
        current = eigvecs
        for low, high, every in groups:
            for panel_index in reversed(range(low, high)):
                vectors = every[panel_index - low, :height]
                factor = every[panel_index - low, height:]
                projected = row_sum(dot(vectors, current, ((0,), (0,))), rows)
                scaled = dot(factor, projected, ((1,), (0,)))
                current = current - dot(vectors, scaled, ((1,), (0,)))
        return current

    in_specs = (P("row", "col"), P(None, "row", "col"), P(None, None, "col"))
    out_specs = P("row", "col")
    return jax.shard_map(local, mesh=mesh, in_specs=in_specs, out_specs=out_specs, check_vma=False)
```
